16 devices in a mesh: dp: 2 (over y, z), tp: 8 (over x, core).
Axes of the slice: x: 4, y: 2, z: 1, core: 2. Of those that a mesh axis runs over, the one named last changes fastest.
The devices are a block of a 4x4x8 slice.
Arguments:
- x: bfloat16 [8192, 2048], P(('dp', 'tp')), parts along dimension 0
- dy: bfloat16 [8192, 2048], P(('dp', 'tp')), parts along dimension 0
- gate: bfloat16 [8192, 16384], P('dp', 'tp'), parts along dimension 0
- up: bfloat16 [8192, 16384], P('dp', 'tp'), parts along dimension 0
- w_gate: bfloat16 [2048, 16384], P(None, 'tp')
- w_up: bfloat16 [2048, 16384], P(None, 'tp')
- w_down: bfloat16 [16384, 2048], P('tp')
Outputs:
- output 1: bfloat16 [8192, 2048], P(('dp', 'tp')), parts along dimension 0
- output 2: bfloat16 [4096, 16384], P('dp', 'tp'), parts along dimension 0
- output 3: bfloat16 [4096, 16384], P('dp', 'tp'), parts along dimension 0
- output 4: bfloat16 [32768, 2048], P(('dp', 'tp')), parts along dimension 0
There are 2 independent parts. The reference program is written for one: setup_inputs(seed, part) draws one part's arguments, and reference() takes and returns one part's arrays. A program takes and returns all parts, laid end to end along the dimension named above; an argument that names none is the same for every part.
All inputs are finite; a program needn't handle non-finite values.
Results may differ from the reference program's by a relative error of at most 0.012.
Values are sent between devices in bfloat16 or wider.
A program may use at most 768 MiB of HBM per device.

```python
import jax
import jax.numpy as jnp

ROWS = 4096
D = 2048
FF = 16384


def act(gate, up):
    return jax.nn.gelu(gate) * up


def setup_inputs(seed: int = 0, part: int = 0) -> dict:
    kx, ky, ka, kb, kg, ku, kd = jax.random.split(jax.random.key(seed), 7)
    kx, ky, ka, kb = (jax.random.fold_in(k, part) for k in (kx, ky, ka, kb))
    drawn = {
        "x": jax.random.normal(kx, (ROWS, D), jnp.float32),
        "dy": jax.random.normal(ky, (ROWS, D), jnp.float32),
        "gate": jax.random.normal(ka, (ROWS, FF), jnp.float32),
        "up": jax.random.normal(kb, (ROWS, FF), jnp.float32),
        "w_gate": jax.random.normal(kg, (D, FF), jnp.float32) * D**-0.5,
        "w_up": jax.random.normal(ku, (D, FF), jnp.float32) * D**-0.5,
        "w_down": jax.random.normal(kd, (FF, D), jnp.float32) * FF**-0.5,
    }
    return {k: v.astype(jnp.bfloat16) for k, v in drawn.items()}


def reference(x, dy, gate, up, w_gate, w_up, w_down):
    hidden, back = jax.vjp(act, gate.astype(jnp.float32), up.astype(jnp.float32))
    d_hidden = jnp.dot(dy, w_down.T, preferred_element_type=jnp.float32)
    d_gate, d_up = (g.astype(jnp.bfloat16) for g in back(d_hidden))
    dx = jnp.dot(d_gate, w_gate.T, preferred_element_type=jnp.float32) + jnp.dot(d_up, w_up.T, preferred_element_type=jnp.float32)
    dw_gate = jnp.dot(x.T, d_gate, preferred_element_type=jnp.float32)
    dw_up = jnp.dot(x.T, d_up, preferred_element_type=jnp.float32)
    dw_down = jnp.dot(hidden.astype(jnp.bfloat16).T, dy, preferred_element_type=jnp.float32)
    return tuple(g.astype(jnp.bfloat16) for g in (dx, dw_gate, dw_up, dw_down))
```

```python
import functools

import jax
import jax.numpy as jnp
from jax import lax
from jax.experimental import pallas as pl
from jax.experimental.pallas import tpu as pltpu
from jax.sharding import PartitionSpec as P

MESH = pl.DeviceIdType.MESH
VMEM_LIMIT = 63 * 2**20
TM = 256
F32, BF16 = jnp.float32, jnp.bfloat16
NT = (((1,), (1,)), ((), ()))
TN = (((0,), (0,)), ((), ()))
ROOT = 0.7978845608028654


def place(i):
    a = i // 4
    mid, far = ((a + 1) // 2) % 2, a // 3
    chip = mid * (2 * (i % 2) - 1) + 2 * far
    half = mid * ((a - 1 + i % 2) % 2) + (1 - mid) * (i % 2)
    return chip, (i // 2) % 2, half


def row_block(i, chips):
    t = lax.axis_index("tp")
    chip, core, half = place(i)
    return ((((t // 2) + chip + chips) % chips) * 2 + (t % 2 + core) % 2) * 2 + half


def backward_act(dh, g, u):
    g2 = g * g
    t = jnp.tanh(ROOT * (g * (1.0 + 0.044715 * g2)))
    cdf = 0.5 + 0.5 * t
    act = g * cdf
    slope = cdf + (0.5 * ROOT) * g * ((1.0 - t * t) * (1.0 + (3 * 0.044715) * g2))
    return act * u, dh * u * slope, dh * act


def kernel_a(chips, dy_ref, x_ref, g_ref, u_ref, wd_ref, wg_ref, wu_ref,
             yx_ref, act_ref, own_ref, other_ref,
             wd, wgu, dybuf, dh, sbuf, w_sem, ld_sem, cp_sem, sdy, rdy, sx, rx, so, ro):
    i = pl.program_id(0)
    steps = pl.num_programs(0)
    t = lax.axis_index("tp")
    n = 2 * chips
    partner = t + 1 - 2 * (t % 2)
    right, left = (t + 2) % n, (t + n - 2) % n
    dp = lax.axis_index("dp")
    ff = wd.shape[0]
    tokens = yx_ref.shape[0] // 2
    dyf_ref, xf_ref = yx_ref.at[pl.ds(0, tokens)], yx_ref.at[pl.ds(tokens, tokens)]

    def tile(ref, j):
        return ref.at[pl.ds(j * TM, TM)]

    def send(src, full, j, to, ssem, rsem):
        return pltpu.make_async_remote_copy(src_ref=src, dst_ref=tile(full, j), send_sem=ssem.at[j], recv_sem=rsem.at[j],
                                            device_id=(dp, to), device_id_type=MESH)

    def arrived(full, j, ssem, rsem):
        send(tile(full, j), full, j, partner, ssem, rsem).wait_recv()

    def hand_over(j):
        k = (j // 4) * 2 + j % 2
        return send(sbuf.at[j % 2], other_ref, k, partner, so, ro)

    def load(src, slot):
        return pltpu.make_async_copy(src, dybuf.at[slot], ld_sem.at[slot])

    w_copies = [
        pltpu.make_async_copy(wd_ref, wd, w_sem.at[0]),
        pltpu.make_async_copy(wg_ref, wgu.at[:, pl.ds(0, ff)], w_sem.at[1]),
        pltpu.make_async_copy(wu_ref, wgu.at[:, pl.ds(ff, ff)], w_sem.at[2]),
    ]
    own_copies = [
        pltpu.make_async_copy(dy_ref, dyf_ref.at[pl.ds(0, 2 * TM)], cp_sem.at[0]),
        pltpu.make_async_copy(x_ref, xf_ref.at[pl.ds(0, 2 * TM)], cp_sem.at[1]),
    ]

    def ring(src, full, ssem, rsem):
        send(tile(src, 0), full, 4, right, ssem, rsem).start()
        send(tile(src, 1), full, 5, left, ssem, rsem).start()
        send(tile(src, 1), full, 8, right, ssem, rsem).start()
        send(tile(src, 0), full, 9, left, ssem, rsem).start()

    def pair(src, full, ssem, rsem):
        send(tile(src, 0), full, 2, partner, ssem, rsem).start()
        send(tile(src, 1), full, 3, partner, ssem, rsem).start()

    @pl.when(i == 0)
    def _():
        w_copies[0].start()
        load(tile(dy_ref, 0), 0).start()
        w_copies[1].start()
        w_copies[2].start()
        barrier = pltpu.get_barrier_semaphore()
        for other in (partner, left, right):
            pl.semaphore_signal(barrier, inc=1, device_id=(dp, other), device_id_type=MESH)
        pl.semaphore_wait(barrier, 3)
        pair(dy_ref, dyf_ref, sdy, rdy)
        ring(dy_ref, dyf_ref, sdy, rdy)
        load(tile(dy_ref, 1), 1).start()
        pair(x_ref, xf_ref, sx, rx)
        for c in own_copies:
            c.start()

    j = i + 1

    @pl.when((j >= 2) & (j < steps))
    def _():
        arrived(dyf_ref, j, sdy, rdy)
        load(tile(dyf_ref, j), j % 2).start()

        @pl.when((j >= 4) & (j % 4 < 2))
        def _():
            send(tile(dyf_ref, j), dyf_ref, j + 2, partner, sdy, rdy).start()

        @pl.when(j == 4)
        def _():
            send(tile(dyf_ref, 4), dyf_ref, 12, right, sdy, rdy).start()

        @pl.when(j == 5)
        def _():
            send(tile(dyf_ref, 5), dyf_ref, 13, left, sdy, rdy).start()

    @pl.when(i == 6)
    def _():
        ring(x_ref, xf_ref, sx, rx)

    @pl.when(i == 12)
    def _():
        for k in (4, 5):
            arrived(xf_ref, k, sx, rx)
            send(tile(xf_ref, k), xf_ref, k + 2, partner, sx, rx).start()
        send(tile(xf_ref, 4), xf_ref, 12, right, sx, rx).start()
        send(tile(xf_ref, 5), xf_ref, 13, left, sx, rx).start()

    @pl.when(i == 15)
    def _():
        for k in (8, 9):
            arrived(xf_ref, k, sx, rx)
            send(tile(xf_ref, k), xf_ref, k + 2, partner, sx, rx).start()

    @pl.when((i >= 3) & ((i - 1) % 4 >= 2))
    def _():
        hand_over(i - 1).start()

    @pl.when((i >= 4) & (i % 4 >= 2))
    def _():
        hand_over(i - 4).wait_send()

    slot = i % 2
    load(tile(dy_ref, 0), slot).wait()

    @pl.when(i == 0)
    def _():
        w_copies[0].wait()

    CB = 256
    for c in range(ff // CB):
        cols = pl.ds(c * CB, CB)
        dh[c % 2] = lax.dot_general(dybuf[slot], wd[cols, :], NT, preferred_element_type=F32)
        for r in range(TM // 32):
            rows = pl.ds(r * 32, 32)
            h, dg, du = backward_act(dh[c % 2, rows, :], g_ref[rows, cols].astype(F32), u_ref[rows, cols].astype(F32))
            act_ref[rows, cols] = h.astype(BF16)
            act_ref[rows, pl.ds(ff + c * CB, CB)] = dg.astype(BF16)
            act_ref[rows, pl.ds(2 * ff + c * CB, CB)] = du.astype(BF16)

    @pl.when(i == 0)
    def _():
        w_copies[1].wait()
        w_copies[2].wait()

    def term(put):
        d = wgu.shape[0]
        NB = 512
        for c in range(d // NB):
            cols = pl.ds(c * NB, NB)
            put(cols, lax.dot_general(act_ref[:, pl.ds(ff, 2 * ff)], wgu[cols, :], NT, preferred_element_type=F32))

    @pl.when(i % 4 < 2)
    def _():
        def put(cols, v):
            own_ref[:, cols] = v
        term(put)

    @pl.when(i % 4 >= 2)
    def _():
        def put(cols, v):
            sbuf[i % 2, :, cols] = v.astype(BF16)
        term(put)

    @pl.when(i == steps - 1)
    def _():
        for k in (12, 13):
            arrived(xf_ref, k, sx, rx)
            send(tile(xf_ref, k), xf_ref, k + 2, partner, sx, rx).start()
        for k in (2, 3, 6, 7, 10, 11, 14, 15):
            arrived(xf_ref, k, sx, rx)
        for k in range(2, 16):
            send(tile(dy_ref, 0), dyf_ref, k, partner, sdy, rdy).wait_send()
            send(tile(x_ref, 0), xf_ref, k, partner, sx, rx).wait_send()
        for c in own_copies:
            c.wait()
        last = hand_over(tokens // TM - 1)
        last.start()
        for k in range(tokens // TM // 2):
            send(sbuf.at[0], other_ref, k, partner, so, ro).wait_recv()
        hand_over(tokens // TM - 2).wait_send()
        last.wait_send()


def call_a(chips, dy, x, gate, up, wd, wg, wu):
    rows, ff = gate.shape
    d = dy.shape[1]
    any_ = pl.BlockSpec(memory_space=pl.ANY)
    kept = pl.BlockSpec((TM, ff), lambda i: (row_block(i, chips), 0))
    return pl.pallas_call(
        functools.partial(kernel_a, chips),
        grid=(rows // TM,),
        in_specs=[any_, any_, kept, kept, any_, any_, any_],
        out_specs=[
            any_,
            pl.BlockSpec((TM, 3 * ff), lambda i: (i, 0)),
            pl.BlockSpec((TM, d), lambda i: ((i // 4) * 2 + (i % 4 + 2) // 3, 0)),
            any_,
        ],
        out_shape=[
            jax.ShapeDtypeStruct((2 * rows, d), BF16), jax.ShapeDtypeStruct((rows, 3 * ff), BF16),
            jax.ShapeDtypeStruct((rows // 2, d), F32), jax.ShapeDtypeStruct((rows // 2, d), BF16),
        ],
        scratch_shapes=[
            pltpu.VMEM((ff, d), BF16), pltpu.VMEM((d, 2 * ff), BF16),
            pltpu.VMEM((2, TM, d), BF16), pltpu.VMEM((2, TM, 256), F32), pltpu.VMEM((2, TM, d), BF16),
            pltpu.SemaphoreType.DMA((3,)), pltpu.SemaphoreType.DMA((2,)), pltpu.SemaphoreType.DMA((2,)),
            pltpu.SemaphoreType.DMA((16,)), pltpu.SemaphoreType.DMA((16,)),
            pltpu.SemaphoreType.DMA((16,)), pltpu.SemaphoreType.DMA((16,)),
            pltpu.SemaphoreType.DMA((8,)), pltpu.SemaphoreType.DMA((8,)),
        ],
        compiler_params=pltpu.CompilerParams(collective_id=0, has_side_effects=True, vmem_limit_bytes=VMEM_LIMIT,
                                             dimension_semantics=("arbitrary",)),
        cost_estimate=pl.CostEstimate(flops=6 * rows * d * ff, bytes_accessed=12 * rows * d, transcendentals=rows * ff),
        name="gather_and_dx",
    )(dy, x, gate, up, wd, wg, wu)


SUB = TM // 2
HOPS = ((2, 3), (6, 7), (5, 4), (0, 1))
EVENTS = [(h, q) for h in range(4) for q in range(2)]
POINTS = (0, 0, 3, 6, 8, 10, 13, 15)


def kernel_b(chips, a_ref, b_ref, own_ref, other_ref, w_ref, dx_ref,
             own, other, come, go, ld_sem, s_sem, r_sem, o_sem):
    s = pl.program_id(0)
    t = lax.axis_index("tp")
    n = 2 * chips
    dp = lax.axis_index("dp")
    ways = ((t + 2) % n, (t + n - 2) % n)

    def loads(e):
        h, q = EVENTS[e]
        for w in range(2):
            at = pl.ds(HOPS[h][w] * TM + q * SUB, SUB)
            yield pltpu.make_async_copy(own_ref.at[at], own.at[e % 2, w], ld_sem.at[e % 2, w, 0])
            yield pltpu.make_async_copy(other_ref.at[at], other.at[e % 2, w], ld_sem.at[e % 2, w, 1])

    def send(e, w):
        return pltpu.make_async_remote_copy(src_ref=go.at[e % 2, w], dst_ref=come.at[e, w], send_sem=s_sem.at[e, w],
                                            recv_sem=r_sem.at[e, w], device_id=(dp, ways[w]), device_id_type=MESH)

    def finish(e, w):
        q = EVENTS[e][1]
        return pltpu.make_async_copy(go.at[e % 2, w], dx_ref.at[pl.ds(w * TM + q * SUB, SUB)], o_sem.at[q, w])

    def event(e):
        h = EVENTS[e][0]
        if e == 0:
            barrier = pltpu.get_barrier_semaphore()
            for c in loads(0):
                c.start()
            for other_ in ways:
                pl.semaphore_signal(barrier, inc=1, device_id=(dp, other_), device_id_type=MESH)
            pl.semaphore_wait(barrier, 2)
        if e + 1 < len(EVENTS):
            for c in loads(e + 1):
                c.start()
        for c in loads(e):
            c.wait()
        for w in range(2):
            if e >= 2:
                send(e - 2, w).wait_recv()
                send(e - 2, w).wait_send()

            @pl.loop(0, SUB // 16)
            def _(r):
                rows = pl.ds(pl.multiple_of(r * 16, 16), 16)
                v = own[e % 2, w, rows, :] + other[e % 2, w, rows, :].astype(F32)
                if e >= 2:
                    v = v + come[e - 2, w, rows, :].astype(F32)
                go[e % 2, w, rows, :] = v.astype(BF16)
        for w in range(2):
            if h < 3:
                send(e, w).start()
            else:
                finish(e, w).start()

    def at_point(half):
        for e, p in enumerate(POINTS):
            if p % 2 == half:
                @pl.when(s == p // 2)
                def _(e=e):
                    event(e)

    for half in range(2):
        at_point(half)

        @pl.when(s < 4)
        def _():
            cols = pl.ds(half * 512, 512)
            w_ref[:, cols] = lax.dot_general(a_ref[...], b_ref[:, cols], TN, preferred_element_type=F32).astype(BF16)

        @pl.when(s >= 4)
        def _():
            cols = pl.ds(half * 512, 512)
            w_ref[:, cols] = lax.dot_general(b_ref[...], a_ref[:, cols], TN, preferred_element_type=F32).astype(BF16)

    @pl.when(s == pl.num_programs(0) - 1)
    def _():
        for e in (6, 7):
            for w in range(2):
                finish(e, w).wait()


def call_b(chips, act, yx, own, other):
    rows, d = act.shape[0], yx.shape[1]
    ff = act.shape[1] // 3
    any_ = pl.BlockSpec(memory_space=pl.ANY)
    q = lambda s: s // 4
    return pl.pallas_call(
        functools.partial(kernel_b, chips),
        grid=(8,),
        in_specs=[
            pl.BlockSpec((rows, ff // 2), lambda s: (0, s // 2)),
            pl.BlockSpec((rows, d // 2), lambda s: (q(s), s % 2)),
            any_, any_,
        ],
        out_specs=[
            pl.BlockSpec((ff // 2, d // 2), lambda s: ((1 - q(s)) * (s // 2) + q(s) * (2 + s % 2), (1 - q(s)) * (s % 2) + q(s) * (s // 2 - 2))),
            any_,
        ],
        out_shape=[jax.ShapeDtypeStruct((ff + d, d), BF16), jax.ShapeDtypeStruct((2 * TM, d), BF16)],
        scratch_shapes=[
            pltpu.VMEM((2, 2, SUB, d), F32), pltpu.VMEM((2, 2, SUB, d), BF16),
            pltpu.VMEM((6, 2, SUB, d), BF16), pltpu.VMEM((2, 2, SUB, d), BF16),
            pltpu.SemaphoreType.DMA((2, 2, 2)), pltpu.SemaphoreType.DMA((6, 2)), pltpu.SemaphoreType.DMA((6, 2)),
            pltpu.SemaphoreType.DMA((2, 2)),
        ],
        compiler_params=pltpu.CompilerParams(collective_id=1, has_side_effects=True, vmem_limit_bytes=VMEM_LIMIT,
                                             dimension_semantics=("arbitrary",)),
        cost_estimate=pl.CostEstimate(flops=4 * rows * d * ff, bytes_accessed=12 * rows * d, transcendentals=0),
        name="scatter_and_dw",
    )(act, yx, own, other)


def call_c(act, yx, w, dx):
    rows, d = act.shape[0], yx.shape[1]
    ff = act.shape[1] // 3

    def kernel(x_ref, du_ref, wd_ref, wg_ref, dx_ref, dx_out, wg_out, wu_out, wd_out):
        for half in range(2):
            cols = pl.ds(half * 512, 512)
            wu_out[:, cols] = lax.dot_general(x_ref[...], du_ref[:, cols], TN, preferred_element_type=F32).astype(BF16)
        dx_out[...] = dx_ref[...]
        wg_out[...] = wg_ref[...]
        wd_out[...] = wd_ref[...]

    return pl.pallas_call(
        kernel,
        grid=(4,),
        in_specs=[
            pl.BlockSpec((rows, d // 2), lambda s: (1, s % 2)),
            pl.BlockSpec((rows, ff // 2), lambda s: (0, 4 + s // 2)),
            pl.BlockSpec((ff // 4, d), lambda s: (s, 0)),
            pl.BlockSpec((d // 4, d), lambda s: (4 + s, 0)),
            pl.BlockSpec((dx.shape[0] // 4, d), lambda s: (s, 0)),
        ],
        out_specs=[
            pl.BlockSpec((dx.shape[0] // 4, d), lambda s: (s, 0)),
            pl.BlockSpec((d // 4, d), lambda s: (s, 0)),
            pl.BlockSpec((d // 2, ff // 2), lambda s: (s % 2, s // 2)),
            pl.BlockSpec((ff // 4, d), lambda s: (s, 0)),
        ],
        out_shape=[jax.ShapeDtypeStruct(dx.shape, BF16), jax.ShapeDtypeStruct((d, ff), BF16),
                   jax.ShapeDtypeStruct((d, ff), BF16), jax.ShapeDtypeStruct((ff, d), BF16)],
        compiler_params=pltpu.CompilerParams(vmem_limit_bytes=VMEM_LIMIT, dimension_semantics=("arbitrary",)),
        cost_estimate=pl.CostEstimate(flops=2 * rows * d * ff, bytes_accessed=12 * rows * d, transcendentals=0),
        name="dw_and_results",
    )(yx, act, w, w, dx)


def solution(mesh):
    chips = mesh.shape["tp"] // 2

    def local(x, dy, gate, up, wg, wu, wd):
        yx, act, own, other = call_a(chips, dy, x, gate, up, wd, wg, wu)
        w, dx = call_b(chips, act, yx, own, other)
        return tuple(call_c(act, yx, w, dx))

    rows, cols = P(("dp", "tp"), None), P("dp", "tp")
    return jax.shard_map(local, mesh=mesh,
                         in_specs=(rows, rows, cols, cols, P(None, "tp"), P(None, "tp"), P("tp", None)),
                         out_specs=(rows, cols, cols, P(("dp", "tp"), None)), check_vma=False)
```

```python
import functools

import jax
import jax.numpy as jnp
from jax import lax
from jax.experimental import pallas as pl
from jax.experimental.pallas import tpu as pltpu
from jax.sharding import PartitionSpec as P

MESH = pl.DeviceIdType.MESH
VMEM_LIMIT = 63 * 2**20
TM = 256
CB = 256
DY_SECOND, DY_FAR, DY_FAR_IN, X_RING, X_FIRST, X_SECOND = 2, 5, 10, (8, 11), 12, 15
F32, BF16 = jnp.float32, jnp.bfloat16
NT = (((1,), (1,)), ((), ()))
TN = (((0,), (0,)), ((), ()))
ROOT, CUBE = 0.7978845608028654, 0.044715


def place(i):
    a = i // 4
    mid, far = ((a + 1) // 2) % 2, a // 3
    chip = mid * (2 * (i % 2) - 1) + 2 * far
    half = mid * ((a - 1 + i % 2) % 2) + (1 - mid) * (i % 2)
    return chip, (i // 2 + far) % 2, half


def row_block(i, chips):
    t = lax.axis_index("tp")
    chip, core, half = place(i)
    return ((((t // 2) + chip + chips) % chips) * 2 + (t % 2 + core) % 2) * 2 + half


def backward_act(dh, g, u):
    g2 = g * g
    t = jnp.tanh(g * (ROOT + (ROOT * CUBE) * g2))
    cdf, rest = 0.5 + 0.5 * t, 0.5 - 0.5 * t
    act = g * cdf
    slope = cdf + act * rest * (2 * ROOT + (6 * ROOT * CUBE) * g2)
    return act * u, dh * u * slope, dh * act


def kernel_a(chips, dy_ref, x_ref, g_ref, u_ref, wd_ref, wg_ref, wu_ref,
             dyf_ref, xf_ref, act_ref, own_ref, other_ref,
             wd, wgu, dybuf, dh, xbuf, sbuf, w_sem, ld_sem, cp_sem, sdy, rdy, sx, rx, so, ro):
    i = pl.program_id(0)
    steps = pl.num_programs(0)
    t = lax.axis_index("tp")
    n = 2 * chips
    partner = t + 1 - 2 * (t % 2)
    right, left = (t + 2) % n, (t + n - 2) % n
    dp = lax.axis_index("dp")
    ff = wd.shape[0]
    tokens = dyf_ref.shape[0]

    def tile(ref, j):
        return ref.at[pl.ds(j * TM, TM)]

    def send(src, full, j, to, ssem, rsem):
        return pltpu.make_async_remote_copy(src_ref=src, dst_ref=tile(full, j), send_sem=ssem.at[j], recv_sem=rsem.at[j],
                                            device_id=(dp, to), device_id_type=MESH)

    def arrived(full, j, ssem, rsem):
        send(tile(full, j), full, j, partner, ssem, rsem).wait_recv()

    def hand_over(j):
        k = (j // 4) * 2 + j % 2
        return send(sbuf.at[j % 2], other_ref, k, partner, so, ro)

    def load(src, slot):
        return pltpu.make_async_copy(src, dybuf.at[slot], ld_sem.at[slot])

    w_copies = [
        pltpu.make_async_copy(wd_ref, wd, w_sem.at[0]),
        pltpu.make_async_copy(wg_ref, wgu.at[:, pl.ds(0, ff)], w_sem.at[1]),
        pltpu.make_async_copy(wu_ref, wgu.at[:, pl.ds(ff, ff)], w_sem.at[2]),
    ]
    x_in = pltpu.make_async_copy(x_ref, xbuf, cp_sem.at[2])
    x_out = pltpu.make_async_copy(xbuf, xf_ref.at[pl.ds(0, 2 * TM)], cp_sem.at[2])

    def put(k):
        return pltpu.make_async_copy(dybuf.at[k], tile(dyf_ref, k), cp_sem.at[k])

    def ring(src, full, ssem, rsem, second):
        send(tile(src, second), full, 4 + 4 * second, right, ssem, rsem).start()
        send(tile(src, 1 - second), full, 5 + 4 * second, left, ssem, rsem).start()

    def pair(src, full, ssem, rsem):
        send(tile(src, 0), full, 2, partner, ssem, rsem).start()
        send(tile(src, 1), full, 3, partner, ssem, rsem).start()

    @pl.when(i == 0)
    def _():
        w_copies[0].start()
        load(tile(dy_ref, 0), 0).start()
        w_copies[1].start()
        w_copies[2].start()
        barrier = pltpu.get_barrier_semaphore()
        for other in (partner, left, right):
            pl.semaphore_signal(barrier, inc=1, device_id=(dp, other), device_id_type=MESH)
        pl.semaphore_wait(barrier, 3)
        pair(dy_ref, dyf_ref, sdy, rdy)
        ring(dy_ref, dyf_ref, sdy, rdy, 0)
        load(tile(dy_ref, 1), 1).start()
        pair(x_ref, xf_ref, sx, rx)

    @pl.when(i == 1)
    def _():
        x_in.start()

    @pl.when(i == 3)
    def _():
        x_in.wait()
        x_out.start()

    @pl.when(i == 5)
    def _():
        x_out.wait()

    j = i + 1

    @pl.when((j >= 2) & (j < 4))
    def _():
        put(j % 2).wait()

    @pl.when((j >= 2) & (j < steps - 2))
    def _():
        arrived(dyf_ref, j, sdy, rdy)

    @pl.when((j >= 2) & (j < steps))
    def _():
        load(tile(dyf_ref, j), j % 2).start()

        @pl.when((j >= 4) & (j < 12) & (j % 4 < 2))
        def _():
            send(tile(dyf_ref, j), dyf_ref, j + 2, partner, sdy, rdy).start()

    @pl.when(i == DY_SECOND)
    def _():
        ring(dy_ref, dyf_ref, sdy, rdy, 1)

    @pl.when(i == DY_FAR)
    def _():
        send(tile(dyf_ref, 4), dyf_ref, 14, right, sdy, rdy).start()
        send(tile(dyf_ref, 5), dyf_ref, 15, left, sdy, rdy).start()

    @pl.when(i == DY_FAR_IN)
    def _():
        for k in (14, 15):
            arrived(dyf_ref, k, sdy, rdy)
            send(tile(dyf_ref, k), dyf_ref, k - 2, partner, sdy, rdy).start()

    for step, second in zip(X_RING, (0, 1)):
        @pl.when(i == step)
        def _(second=second):
            ring(x_ref, xf_ref, sx, rx, second)

    @pl.when((i == X_FIRST) | (i == X_SECOND))
    def _():
        for k in (4, 5):
            k = k + 4 * (i // X_SECOND)
            arrived(xf_ref, k, sx, rx)
            send(tile(xf_ref, k), xf_ref, k + 2, partner, sx, rx).start()

    def for_partner(k):
        return (k >= 0) & ((k // 2 + k // 12) % 2 == 1)

    @pl.when(for_partner(i - 1))
    def _():
        hand_over(i - 1).start()

    @pl.when(for_partner(i - 2))
    def _():
        hand_over(i - 2).wait_send()

    slot = i % 2
    load(tile(dy_ref, 0), slot).wait()

    @pl.when(i < 2)
    def _():
        put(slot).start()

    def first(c):
        cols = pl.ds(pl.multiple_of(c * CB, CB), CB)
        dh[c % 2] = lax.dot_general(dybuf[slot], wd[cols, :], NT, preferred_element_type=F32)
        for r in range(TM // 32):
            part = pl.ds(r * 32, 32)
            values = backward_act(dh[c % 2, part, :], g_ref[part, cols].astype(F32), u_ref[part, cols].astype(F32))
            for k, v in enumerate(values):
                act_ref[part, pl.ds(pl.multiple_of(k * ff + c * CB, CB), CB)] = v.astype(BF16)

    def second(c, width):
        cols = pl.ds(pl.multiple_of(c * width, width), width)
        v = lax.dot_general(act_ref[:, pl.ds(ff, 2 * ff)], wgu[cols, :], NT, preferred_element_type=F32)
        own_ref[:, cols] = v
        sbuf[slot, :, cols] = v.astype(BF16)

    @pl.when(i == 0)
    def _():
        w_copies[0].wait()
        pl.loop(0, ff // CB)(first)
        w_copies[1].wait()
        w_copies[2].wait()
        pl.loop(0, wgu.shape[0] // 512)(lambda c: second(c, 512))

    @pl.when(i > 0)
    def _():
        for c in range(ff // CB):
            first(c)
        second(0, wgu.shape[0])

    @pl.when(i == steps - 1)
    def _():
        for k in (2, 3, 6, 7, 10, 11):
            arrived(xf_ref, k, sx, rx)
        for k in range(2, 16):
            send(tile(dy_ref, 0), dyf_ref, k, partner, sdy, rdy).wait_send()
        for k in range(2, 12):
            send(tile(x_ref, 0), xf_ref, k, partner, sx, rx).wait_send()
        for k in range(tokens // TM // 2):
            send(sbuf.at[0], other_ref, k, partner, so, ro).wait_recv()


def call_a(chips, dy, x, gate, up, wd, wg, wu):
    rows, ff = gate.shape
    d = dy.shape[1]
    any_ = pl.BlockSpec(memory_space=pl.ANY)
    kept = pl.BlockSpec((TM, ff), lambda i: (row_block(i, chips), 0))
    return pl.pallas_call(
        functools.partial(kernel_a, chips),
        grid=(rows // TM,),
        in_specs=[any_, any_, kept, kept, any_, any_, any_],
        out_specs=[
            any_, any_,
            pl.BlockSpec((TM, 3 * ff), lambda i: (i, 0)),
            pl.BlockSpec((TM, d), lambda i: (i, 0)),
            any_,
        ],
        out_shape=[
            jax.ShapeDtypeStruct((rows, d), BF16), jax.ShapeDtypeStruct((rows * 3 // 4, d), BF16),
            jax.ShapeDtypeStruct((rows, 3 * ff), BF16),
            jax.ShapeDtypeStruct((rows, d), F32), jax.ShapeDtypeStruct((rows // 2, d), BF16),
        ],
        scratch_shapes=[
            pltpu.VMEM((ff, d), BF16), pltpu.VMEM((d, 2 * ff), BF16),
            pltpu.VMEM((2, TM, d), BF16), pltpu.VMEM((2, TM, CB), F32), pltpu.VMEM((2 * TM, d), BF16), pltpu.VMEM((2, TM, d), BF16),
            pltpu.SemaphoreType.DMA((3,)), pltpu.SemaphoreType.DMA((2,)), pltpu.SemaphoreType.DMA((3,)),
            pltpu.SemaphoreType.DMA((16,)), pltpu.SemaphoreType.DMA((16,)),
            pltpu.SemaphoreType.DMA((16,)), pltpu.SemaphoreType.DMA((16,)),
            pltpu.SemaphoreType.DMA((8,)), pltpu.SemaphoreType.DMA((8,)),
        ],
        compiler_params=pltpu.CompilerParams(collective_id=0, has_side_effects=True, vmem_limit_bytes=VMEM_LIMIT,
                                             dimension_semantics=("arbitrary",)),
        cost_estimate=pl.CostEstimate(flops=6 * rows * d * ff, bytes_accessed=12 * rows * d, transcendentals=rows * ff),
        name="gather_and_dx",
    )(dy, x, gate, up, wd, wg, wu)


SUB = TM // 2
HOPS = ((4, 14, 9, 0), (5, 15, 8, 1))
FAR_STEP = 3


def kernel_b(chips, a_ref, dyf_ref, xn_ref, own_ref, other_ref, w_ref, dx_ref, xfar_ref,
             b_buf, own, other, come, go, b_sem, ld_sem, s_sem, r_sem, o_sem, sf, rf):
    s = pl.program_id(0)
    last = pl.num_programs(0) - 1
    t = lax.axis_index("tp")
    n = 2 * chips
    dp = lax.axis_index("dp")
    partner = t + 1 - 2 * (t % 2)
    ways = ((t + 2) % n, (t + n - 2) % n)
    near = xn_ref.shape[0]
    half_d = b_buf.shape[2]

    def fetch_dy(k):
        cols = pl.ds(pl.multiple_of((k % 2) * half_d, half_d), half_d)
        return pltpu.make_async_copy(dyf_ref.at[:, cols], b_buf.at[k % 2], b_sem.at[k % 2, 0])

    def fetch_near(k):
        cols = pl.ds(pl.multiple_of((k % 2) * half_d, half_d), half_d)
        return pltpu.make_async_copy(xn_ref.at[:, cols], b_buf.at[k % 2, pl.ds(0, near)], b_sem.at[k % 2, 0])

    def fetch_far(k):
        cols = pl.ds(pl.multiple_of((k % 2) * half_d, half_d), half_d)
        far = b_buf.shape[1] - near
        return pltpu.make_async_copy(xfar_ref.at[:, cols], b_buf.at[k % 2, pl.ds(near, far)], b_sem.at[k % 2, 1])

    def fetch_x(k):
        return fetch_near(k), fetch_far(k)

    def far_send(k):
        src = xn_ref.at[pl.ds((4 + k) * TM, TM)] if k < 2 else xfar_ref.at[pl.ds(k * TM, TM)]
        to = ways[k] if k < 2 else partner
        return pltpu.make_async_remote_copy(src_ref=src, dst_ref=xfar_ref.at[pl.ds((k + 2) % 4 * TM, TM)], send_sem=sf.at[k],
                                            recv_sem=rf.at[k], device_id=(dp, to), device_id_type=MESH)

    def joins(w, h):
        odd, high = h % 2, h // 2
        k0, k1, k2, k3 = HOPS[w]
        return (1 - odd) * (1 - high) * k0 + odd * (1 - high) * k1 + (1 - odd) * high * k2 + odd * high * k3

    def loads(e):
        for w in range(2):
            k = joins(w, e // 2)
            at = pl.ds(pl.multiple_of(k * TM + (e % 2) * SUB, SUB), SUB)
            yield pltpu.make_async_copy(own_ref.at[at], own.at[e % 2, w], ld_sem.at[e % 2, w, 0])
            at = pl.ds(pl.multiple_of(((k // 4) * 2 + k % 2) * TM + (e % 2) * SUB, SUB), SUB)
            yield pltpu.make_async_copy(other_ref.at[at], other.at[e % 2, w], ld_sem.at[e % 2, w, 1])

    def send(e, w):
        return pltpu.make_async_remote_copy(src_ref=go.at[e % 2, w], dst_ref=come.at[e, w], send_sem=s_sem.at[e, w],
                                            recv_sem=r_sem.at[e, w], device_id=(dp, ways[w]), device_id_type=MESH)

    def finish(e, w):
        at = pl.ds(pl.multiple_of(w * TM + (e % 2) * SUB, SUB), SUB)
        return pltpu.make_async_copy(go.at[e % 2, w], dx_ref.at[at], o_sem.at[e % 2, w])

    def add(e, carried):
        for w in range(2):
            for r in range(SUB // 16):
                rows = pl.ds(r * 16, 16)
                v = own[e % 2, w, rows, :] + other[e % 2, w, rows, :].astype(F32)
                if carried:
                    v = v + come[e - 2, w, rows, :].astype(F32)
                go[e % 2, w, rows, :] = v.astype(BF16)

    def event(e):
        for c in loads(e):
            c.wait()

        @pl.when(e < 7)
        def _():
            for c in loads(e + 1):
                c.start()

        @pl.when(e < 2)
        def _():
            add(e, False)

        @pl.when(e >= 2)
        def _():
            for w in range(2):
                send(e - 2, w).wait_recv()
                send(e - 2, w).wait_send()
            add(e, True)

        @pl.when(e < 6)
        def _():
            for w in range(2):
                send(e, w).start()

        @pl.when(e >= 6)
        def _():
            for w in range(2):
                finish(e, w).start()

    @pl.when(s == 0)
    def _():
        fetch_dy(0).start()
        for c in loads(0):
            c.start()
        barrier = pltpu.get_barrier_semaphore()
        for peer in (partner, *ways):
            pl.semaphore_signal(barrier, inc=1, device_id=(dp, peer), device_id_type=MESH)
        pl.semaphore_wait(barrier, 3)
        for k in (0, 1):
            far_send(k).start()
        fetch_dy(0).wait()

    @pl.when((s > 0) & (s < 4))
    def _():
        fetch_dy(s).wait()

    @pl.when(s == FAR_STEP + 1)
    def _():
        for k in (2, 3):
            far_send(k).wait_recv()
        fetch_far(s).start()

    @pl.when((s >= 4) & (s < last))
    def _():
        for c in fetch_x(s):
            c.wait()

    @pl.when(s < 3)
    def _():
        fetch_dy(s + 1).start()

    @pl.when(s == FAR_STEP)
    def _():
        for k in (0, 1):
            far_send(k).wait_recv()
            far_send(k + 2).start()
        fetch_near(s + 1).start()

    @pl.when((s > FAR_STEP) & (s < last - 1))
    def _():
        for c in fetch_x(s + 1):
            c.start()

    @pl.when((s > 0) & (s % 4 < 3))
    def _():
        event(s - 1 - s // 4)

    slot = s % 2

    @pl.when(s < 4)
    def _():
        w_ref[...] = lax.dot_general(a_ref[...], b_buf[slot], TN, preferred_element_type=F32).astype(BF16)

    @pl.when((s >= 4) & (s < last))
    def _():
        w_ref[...] = lax.dot_general(b_buf[slot], a_ref[...], TN, preferred_element_type=F32).astype(BF16)

    @pl.when(s == last)
    def _():
        for k in range(4):
            far_send(k).wait_send()
        for e in (6, 7):
            for w in range(2):
                finish(e, w).wait()


def call_b(chips, act, dyf, xn, own, other):
    rows, d = dyf.shape
    ff = act.shape[1] // 3
    any_ = pl.BlockSpec(memory_space=pl.ANY)
    x_part = lambda s: jnp.minimum(s // 4, 1)

    def block(s):
        s = jnp.minimum(s, 9)
        x = x_part(s)
        return (1 - x) * (s // 2) + x * (2 * (s // 4) + s % 2), (1 - x) * (s % 2) + x * ((s // 2) % 2)

    return pl.pallas_call(
        functools.partial(kernel_b, chips),
        grid=(11,),
        in_specs=[pl.BlockSpec((rows, ff // 2), lambda s: (0, jnp.minimum(s, 9) // 2)), any_, any_, any_, any_],
        out_specs=[pl.BlockSpec((d // 2, d // 2), block), any_, any_],
        out_shape=[jax.ShapeDtypeStruct((ff + 2 * d, d), BF16), jax.ShapeDtypeStruct((2 * TM, d), BF16),
                   jax.ShapeDtypeStruct((rows // 4, d), BF16)],
        scratch_shapes=[
            pltpu.VMEM((2, rows, d // 2), BF16),
            pltpu.VMEM((2, 2, SUB, d), F32), pltpu.VMEM((2, 2, SUB, d), BF16),
            pltpu.VMEM((6, 2, SUB, d), BF16), pltpu.VMEM((2, 2, SUB, d), BF16),
            pltpu.SemaphoreType.DMA((2, 2)),
            pltpu.SemaphoreType.DMA((2, 2, 2)), pltpu.SemaphoreType.DMA((6, 2)), pltpu.SemaphoreType.DMA((6, 2)),
            pltpu.SemaphoreType.DMA((2, 2)), pltpu.SemaphoreType.DMA((4,)), pltpu.SemaphoreType.DMA((4,)),
        ],
        compiler_params=pltpu.CompilerParams(collective_id=1, has_side_effects=True, vmem_limit_bytes=VMEM_LIMIT,
                                             dimension_semantics=("arbitrary",)),
        cost_estimate=pl.CostEstimate(flops=5 * rows * d * ff, bytes_accessed=12 * rows * d, transcendentals=0),
        name="scatter_and_dw",
    )(act, dyf, xn, own, other)


def call_c(act, xn, xfar, w, dx):
    rows, d = act.shape[0], xn.shape[1]
    ff = act.shape[1] // 3
    near = xn.shape[0]
    cut = 4

    def kernel(xn_ref, xfar_ref, du_ref, wd_ref, wg_ref, wu_ref, dx_ref, dx_out, wg_out, wu_out, wd_out):
        dx_out[...] = dx_ref[...]
        wg_out[...] = wg_ref[...]
        wd_out[...] = wd_ref[...]
        wu_out[:, :ff // 2] = wu_ref[...]
        v = lax.dot_general(xn_ref[...], du_ref[:near], TN, preferred_element_type=F32)
        v = v + lax.dot_general(xfar_ref[...], du_ref[near:], TN, preferred_element_type=F32)
        wu_out[:, ff // 2:] = v.astype(BF16)

    rows_of = lambda size, start=0: pl.BlockSpec((size // cut, d), lambda s: (start + s, 0))
    return pl.pallas_call(
        kernel,
        grid=(cut,),
        in_specs=[
            pl.BlockSpec((near, d // cut), lambda s: (0, s)),
            pl.BlockSpec((rows - near, d // cut), lambda s: (0, s)),
            pl.BlockSpec((rows, ff // 2), lambda s: (0, 5)),
            rows_of(ff), rows_of(d, cut),
            pl.BlockSpec((d // cut, ff // 2), lambda s: (2 * cut + s, 0)),
            rows_of(dx.shape[0]),
        ],
        out_specs=[rows_of(dx.shape[0]), rows_of(d), rows_of(d), rows_of(ff)],
        out_shape=[jax.ShapeDtypeStruct(dx.shape, BF16), jax.ShapeDtypeStruct((d, ff), BF16),
                   jax.ShapeDtypeStruct((d, ff), BF16), jax.ShapeDtypeStruct((ff, d), BF16)],
        compiler_params=pltpu.CompilerParams(vmem_limit_bytes=VMEM_LIMIT, dimension_semantics=("arbitrary",)),
        cost_estimate=pl.CostEstimate(flops=rows * d * ff, bytes_accessed=12 * rows * d, transcendentals=0),
        name="dw_and_results",
    )(xn, xfar, act, w, w, w, dx)


def solution(mesh):
    chips = mesh.shape["tp"] // 2

    def local(x, dy, gate, up, wg, wu, wd):
        dyf, xn, act, own, other = call_a(chips, dy, x, gate, up, wd, wg, wu)
        w, dx, xfar = call_b(chips, act, dyf, xn, own, other)
        return tuple(call_c(act, xn, xfar, w, dx))

    rows, cols = P(("dp", "tp"), None), P("dp", "tp")
    return jax.shard_map(local, mesh=mesh,
                         in_specs=(rows, rows, cols, cols, P(None, "tp"), P(None, "tp"), P("tp", None)),
                         out_specs=(rows, cols, cols, P(("dp", "tp"), None)), check_vma=False)
```

```python
import functools

import jax
import jax.numpy as jnp
from jax import lax
from jax.experimental import pallas as pl
from jax.experimental.pallas import tpu as pltpu
from jax.sharding import PartitionSpec as P

MESH = pl.DeviceIdType.MESH
VMEM_LIMIT = 63 * 2**20
TM = 256
CB, NB = 256, 512
DY_SECOND, DY_FAR, DY_FAR_IN, X_RING, X_FIRST, X_SECOND = 2, 5, 10, (8, 11), 12, 15
F32, BF16 = jnp.float32, jnp.bfloat16
NT = (((1,), (1,)), ((), ()))
TN = (((0,), (0,)), ((), ()))
ROOT, CUBE = 0.7978845608028654, 0.044715


def place(i):
    a = i // 4
    mid, far = ((a + 1) // 2) % 2, a // 3
    chip = mid * (2 * (i % 2) - 1) + 2 * far
    half = mid * ((a - 1 + i % 2) % 2) + (1 - mid) * (i % 2)
    return chip, (i // 2 + far) % 2, half


def row_block(i, chips):
    t = lax.axis_index("tp")
    chip, core, half = place(i)
    return ((((t // 2) + chip + chips) % chips) * 2 + (t % 2 + core) % 2) * 2 + half


def backward_act(dh, g, u):
    g2 = g * g
    t = jnp.tanh(g * (ROOT + (ROOT * CUBE) * g2))
    cdf, rest = 0.5 + 0.5 * t, 0.5 - 0.5 * t
    act = g * cdf
    slope = cdf + act * rest * (2 * ROOT + (6 * ROOT * CUBE) * g2)
    return act * u, dh * u * slope, dh * act


def kernel_a(chips, dy_ref, x_ref, g_ref, u_ref, wd_ref, wg_ref, wu_ref,
             dyf_ref, xf_ref, act_ref, own_ref, other_ref,
             wd, wgu, dybuf, dh, xbuf, sbuf, w_sem, ld_sem, cp_sem, sdy, rdy, sx, rx, so, ro):
    i = pl.program_id(0)
    steps = pl.num_programs(0)
    t = lax.axis_index("tp")
    n = 2 * chips
    partner = t + 1 - 2 * (t % 2)
    right, left = (t + 2) % n, (t + n - 2) % n
    dp = lax.axis_index("dp")
    ff = wd.shape[0]
    tokens = dyf_ref.shape[0]

    def tile(ref, j):
        return ref.at[pl.ds(j * TM, TM)]

    def send(src, full, j, to, ssem, rsem):
        return pltpu.make_async_remote_copy(src_ref=src, dst_ref=tile(full, j), send_sem=ssem.at[j], recv_sem=rsem.at[j],
                                            device_id=(dp, to), device_id_type=MESH)

    def arrived(full, j, ssem, rsem):
        send(tile(full, j), full, j, partner, ssem, rsem).wait_recv()

    def hand_over(j):
        k = (j // 4) * 2 + j % 2
        return send(sbuf.at[j % 2], other_ref, k, partner, so, ro)

    def load(src, slot):
        return pltpu.make_async_copy(src, dybuf.at[slot], ld_sem.at[slot])

    def load_down(c):
        at = pl.ds(pl.multiple_of(c * CB, CB), CB)
        return pltpu.make_async_copy(wd_ref.at[at], wd.at[at], w_sem.at[0, c])

    def load_gate_up(c):
        at = pl.ds(pl.multiple_of(c * NB, NB), NB)
        return (pltpu.make_async_copy(wg_ref.at[at], wgu.at[at, pl.ds(0, ff)], w_sem.at[1, c]),
                pltpu.make_async_copy(wu_ref.at[at], wgu.at[at, pl.ds(ff, ff)], w_sem.at[2, c]))

    x_in = pltpu.make_async_copy(x_ref, xbuf, cp_sem.at[2])
    x_out = pltpu.make_async_copy(xbuf, xf_ref.at[pl.ds(0, 2 * TM)], cp_sem.at[2])

    def put(k):
        return pltpu.make_async_copy(dybuf.at[k], tile(dyf_ref, k), cp_sem.at[k])

    def ring(src, full, ssem, rsem, second):
        send(tile(src, second), full, 4 + 4 * second, right, ssem, rsem).start()
        send(tile(src, 1 - second), full, 5 + 4 * second, left, ssem, rsem).start()

    def pair(src, full, ssem, rsem):
        send(tile(src, 0), full, 2, partner, ssem, rsem).start()
        send(tile(src, 1), full, 3, partner, ssem, rsem).start()

    @pl.when(i == 0)
    def _():
        load(tile(dy_ref, 0), 0).start()
        pl.loop(0, ff // CB)(lambda c: load_down(c).start())

        @pl.loop(0, wgu.shape[0] // NB)
        def _(c):
            for copy in load_gate_up(c):
                copy.start()

        barrier = pltpu.get_barrier_semaphore()
        for other in (partner, left, right):
            pl.semaphore_signal(barrier, inc=1, device_id=(dp, other), device_id_type=MESH)
        pl.semaphore_wait(barrier, 3)
        pair(dy_ref, dyf_ref, sdy, rdy)
        ring(dy_ref, dyf_ref, sdy, rdy, 0)
        load(tile(dy_ref, 1), 1).start()
        pair(x_ref, xf_ref, sx, rx)

    @pl.when(i == 1)
    def _():
        x_in.start()

    @pl.when(i == 3)
    def _():
        x_in.wait()
        x_out.start()

    @pl.when(i == 5)
    def _():
        x_out.wait()

    j = i + 1

    @pl.when((j >= 2) & (j < 4))
    def _():
        put(j % 2).wait()

    @pl.when((j >= 2) & (j < steps - 2))
    def _():
        arrived(dyf_ref, j, sdy, rdy)

    @pl.when((j >= 2) & (j < steps))
    def _():
        load(tile(dyf_ref, j), j % 2).start()

        @pl.when((j >= 4) & (j < 12) & (j % 4 < 2))
        def _():
            send(tile(dyf_ref, j), dyf_ref, j + 2, partner, sdy, rdy).start()

    @pl.when(i == DY_SECOND)
    def _():
        ring(dy_ref, dyf_ref, sdy, rdy, 1)

    @pl.when(i == DY_FAR)
    def _():
        send(tile(dyf_ref, 4), dyf_ref, 14, right, sdy, rdy).start()
        send(tile(dyf_ref, 5), dyf_ref, 15, left, sdy, rdy).start()

    @pl.when(i == DY_FAR_IN)
    def _():
        for k in (14, 15):
            arrived(dyf_ref, k, sdy, rdy)
            send(tile(dyf_ref, k), dyf_ref, k - 2, partner, sdy, rdy).start()

    for step, second in zip(X_RING, (0, 1)):
        @pl.when(i == step)
        def _(second=second):
            ring(x_ref, xf_ref, sx, rx, second)

    @pl.when((i == X_FIRST) | (i == X_SECOND))
    def _():
        for k in (4, 5):
            k = k + 4 * (i // X_SECOND)
            arrived(xf_ref, k, sx, rx)
            send(tile(xf_ref, k), xf_ref, k + 2, partner, sx, rx).start()

    def for_partner(k):
        return (k >= 0) & ((k // 2 + k // 12) % 2 == 1)

    @pl.when(for_partner(i - 1))
    def _():
        hand_over(i - 1).start()

    @pl.when(for_partner(i - 2))
    def _():
        hand_over(i - 2).wait_send()

    slot = i % 2
    load(tile(dy_ref, 0), slot).wait()

    @pl.when(i < 2)
    def _():
        put(slot).start()

    def first(c):
        cols = pl.ds(pl.multiple_of(c * CB, CB), CB)
        dh[c % 2] = lax.dot_general(dybuf[slot], wd[cols, :], NT, preferred_element_type=F32)
        for r in range(TM // 32):
            part = pl.ds(r * 32, 32)
            values = backward_act(dh[c % 2, part, :], g_ref[part, cols].astype(F32), u_ref[part, cols].astype(F32))
            for k, v in enumerate(values):
                act_ref[part, pl.ds(pl.multiple_of(k * ff + c * CB, CB), CB)] = v.astype(BF16)

    def second(c, width):
        cols = pl.ds(pl.multiple_of(c * width, width), width)
        v = lax.dot_general(act_ref[:, pl.ds(ff, 2 * ff)], wgu[cols, :], NT, preferred_element_type=F32)
        own_ref[:, cols] = v
        sbuf[slot, :, cols] = v.astype(BF16)

    @pl.when(i == 0)
    def _():
        @pl.loop(0, ff // CB)
        def _(c):
            load_down(c).wait()
            first(c)

        @pl.loop(0, wgu.shape[0] // NB)
        def _(c):
            for copy in load_gate_up(c):
                copy.wait()
            second(c, NB)

    @pl.when(i > 0)
    def _():
        for c in range(ff // CB):
            first(c)
        second(0, wgu.shape[0])

    @pl.when(i == steps - 1)
    def _():
        for k in (2, 3, 6, 7, 10, 11):
            arrived(xf_ref, k, sx, rx)
        for k in range(2, 16):
            send(tile(dy_ref, 0), dyf_ref, k, partner, sdy, rdy).wait_send()
        for k in range(2, 12):
            send(tile(x_ref, 0), xf_ref, k, partner, sx, rx).wait_send()
        for k in range(tokens // TM // 2):
            send(sbuf.at[0], other_ref, k, partner, so, ro).wait_recv()


def call_a(chips, dy, x, gate, up, wd, wg, wu):
    rows, ff = gate.shape
    d = dy.shape[1]
    any_ = pl.BlockSpec(memory_space=pl.ANY)
    kept = pl.BlockSpec((TM, ff), lambda i: (row_block(i, chips), 0))
    return pl.pallas_call(
        functools.partial(kernel_a, chips),
        grid=(rows // TM,),
        in_specs=[any_, any_, kept, kept, any_, any_, any_],
        out_specs=[
            any_, any_,
            pl.BlockSpec((TM, 3 * ff), lambda i: (i, 0)),
            pl.BlockSpec((TM, d), lambda i: (i, 0)),
            any_,
        ],
        out_shape=[
            jax.ShapeDtypeStruct((rows, d), BF16), jax.ShapeDtypeStruct((rows * 3 // 4, d), BF16),
            jax.ShapeDtypeStruct((rows, 3 * ff), BF16),
            jax.ShapeDtypeStruct((rows, d), F32), jax.ShapeDtypeStruct((rows // 2, d), BF16),
        ],
        scratch_shapes=[
            pltpu.VMEM((ff, d), BF16), pltpu.VMEM((d, 2 * ff), BF16),
            pltpu.VMEM((2, TM, d), BF16), pltpu.VMEM((2, TM, CB), F32), pltpu.VMEM((2 * TM, d), BF16), pltpu.VMEM((2, TM, d), BF16),
            pltpu.SemaphoreType.DMA((3, 8)), pltpu.SemaphoreType.DMA((2,)), pltpu.SemaphoreType.DMA((3,)),
            pltpu.SemaphoreType.DMA((16,)), pltpu.SemaphoreType.DMA((16,)),
            pltpu.SemaphoreType.DMA((16,)), pltpu.SemaphoreType.DMA((16,)),
            pltpu.SemaphoreType.DMA((8,)), pltpu.SemaphoreType.DMA((8,)),
        ],
        compiler_params=pltpu.CompilerParams(collective_id=0, has_side_effects=True, vmem_limit_bytes=VMEM_LIMIT,
                                             dimension_semantics=("arbitrary",)),
        cost_estimate=pl.CostEstimate(flops=6 * rows * d * ff, bytes_accessed=12 * rows * d, transcendentals=rows * ff),
        name="gather_and_dx",
    )(dy, x, gate, up, wd, wg, wu)


SUB = TM // 2
HOPS = ((4, 14, 9, 0), (5, 15, 8, 1))
FAR_STEP = 3


def kernel_b(chips, a_ref, dyf_ref, xn_ref, own_ref, other_ref, w_ref, dx_ref, xfar_ref,
             b_buf, own, other, come, go, b_sem, ld_sem, s_sem, r_sem, o_sem, sf, rf):
    s = pl.program_id(0)
    last = pl.num_programs(0) - 1
    t = lax.axis_index("tp")
    n = 2 * chips
    dp = lax.axis_index("dp")
    partner = t + 1 - 2 * (t % 2)
    ways = ((t + 2) % n, (t + n - 2) % n)
    near = xn_ref.shape[0]
    half_d = b_buf.shape[2]

    def fetch_dy(k):
        cols = pl.ds(pl.multiple_of((k % 2) * half_d, half_d), half_d)
        return pltpu.make_async_copy(dyf_ref.at[:, cols], b_buf.at[k % 2], b_sem.at[k % 2, 0])

    def fetch_near(k):
        cols = pl.ds(pl.multiple_of((k % 2) * half_d, half_d), half_d)
        return pltpu.make_async_copy(xn_ref.at[:, cols], b_buf.at[k % 2, pl.ds(0, near)], b_sem.at[k % 2, 0])

    def fetch_far(k):
        cols = pl.ds(pl.multiple_of((k % 2) * half_d, half_d), half_d)
        far = b_buf.shape[1] - near
        return pltpu.make_async_copy(xfar_ref.at[:, cols], b_buf.at[k % 2, pl.ds(near, far)], b_sem.at[k % 2, 1])

    def fetch_x(k):
        return fetch_near(k), fetch_far(k)

    def far_send(k):
        src = xn_ref.at[pl.ds((4 + k) * TM, TM)] if k < 2 else xfar_ref.at[pl.ds(k * TM, TM)]
        to = ways[k] if k < 2 else partner
        return pltpu.make_async_remote_copy(src_ref=src, dst_ref=xfar_ref.at[pl.ds((k + 2) % 4 * TM, TM)], send_sem=sf.at[k],
                                            recv_sem=rf.at[k], device_id=(dp, to), device_id_type=MESH)

    def joins(w, h):
        odd, high = h % 2, h // 2
        k0, k1, k2, k3 = HOPS[w]
        return (1 - odd) * (1 - high) * k0 + odd * (1 - high) * k1 + (1 - odd) * high * k2 + odd * high * k3

    def loads(e):
        for w in range(2):
            k = joins(w, e // 2)
            at = pl.ds(pl.multiple_of(k * TM + (e % 2) * SUB, SUB), SUB)
            yield pltpu.make_async_copy(own_ref.at[at], own.at[e % 2, w], ld_sem.at[e % 2, w, 0])
            at = pl.ds(pl.multiple_of(((k // 4) * 2 + k % 2) * TM + (e % 2) * SUB, SUB), SUB)
            yield pltpu.make_async_copy(other_ref.at[at], other.at[e % 2, w], ld_sem.at[e % 2, w, 1])

    def send(e, w):
        return pltpu.make_async_remote_copy(src_ref=go.at[e % 2, w], dst_ref=come.at[e, w], send_sem=s_sem.at[e, w],
                                            recv_sem=r_sem.at[e, w], device_id=(dp, ways[w]), device_id_type=MESH)

    def finish(e, w):
        at = pl.ds(pl.multiple_of(w * TM + (e % 2) * SUB, SUB), SUB)
        return pltpu.make_async_copy(go.at[e % 2, w], dx_ref.at[at], o_sem.at[e % 2, w])

    def add(e, carried):
        for w in range(2):
            for r in range(SUB // 16):
                rows = pl.ds(r * 16, 16)
                v = own[e % 2, w, rows, :] + other[e % 2, w, rows, :].astype(F32)
                if carried:
                    v = v + come[e - 2, w, rows, :].astype(F32)
                go[e % 2, w, rows, :] = v.astype(BF16)

    def event(e):
        for c in loads(e):
            c.wait()

        @pl.when(e < 7)
        def _():
            for c in loads(e + 1):
                c.start()

        @pl.when(e < 2)
        def _():
            add(e, False)

        @pl.when(e >= 2)
        def _():
            for w in range(2):
                send(e - 2, w).wait_recv()
                send(e - 2, w).wait_send()
            add(e, True)

        @pl.when(e < 6)
        def _():
            for w in range(2):
                send(e, w).start()

        @pl.when(e >= 6)
        def _():
            for w in range(2):
                finish(e, w).start()

    @pl.when(s == 0)
    def _():
        fetch_dy(0).start()
        for c in loads(0):
            c.start()
        barrier = pltpu.get_barrier_semaphore()
        for peer in (partner, *ways):
            pl.semaphore_signal(barrier, inc=1, device_id=(dp, peer), device_id_type=MESH)
        pl.semaphore_wait(barrier, 3)
        for k in (0, 1):
            far_send(k).start()
        fetch_dy(0).wait()

    @pl.when((s > 0) & (s < 4))
    def _():
        fetch_dy(s).wait()

    @pl.when(s == FAR_STEP + 1)
    def _():
        for k in (2, 3):
            far_send(k).wait_recv()
        fetch_far(s).start()

    @pl.when((s >= 4) & (s < last))
    def _():
        for c in fetch_x(s):
            c.wait()

    @pl.when(s < 3)
    def _():
        fetch_dy(s + 1).start()

    @pl.when(s == FAR_STEP)
    def _():
        for k in (0, 1):
            far_send(k).wait_recv()
            far_send(k + 2).start()
        fetch_near(s + 1).start()

    @pl.when((s > FAR_STEP) & (s < last - 1))
    def _():
        for c in fetch_x(s + 1):
            c.start()

    @pl.when((s > 0) & (s % 4 < 3))
    def _():
        event(s - 1 - s // 4)

    slot = s % 2

    @pl.when(s < 4)
    def _():
        w_ref[...] = lax.dot_general(a_ref[...], b_buf[slot], TN, preferred_element_type=F32).astype(BF16)

    @pl.when((s >= 4) & (s < last))
    def _():
        w_ref[...] = lax.dot_general(b_buf[slot], a_ref[...], TN, preferred_element_type=F32).astype(BF16)

    @pl.when(s == last)
    def _():
        for k in range(4):
            far_send(k).wait_send()
        for e in (6, 7):
            for w in range(2):
                finish(e, w).wait()


def call_b(chips, act, dyf, xn, own, other):
    rows, d = dyf.shape
    ff = act.shape[1] // 3
    any_ = pl.BlockSpec(memory_space=pl.ANY)
    x_part = lambda s: jnp.minimum(s // 4, 1)

    def block(s):
        s = jnp.minimum(s, 9)
        x = x_part(s)
        return (1 - x) * (s // 2) + x * (2 * (s // 4) + s % 2), (1 - x) * (s % 2) + x * ((s // 2) % 2)

    return pl.pallas_call(
        functools.partial(kernel_b, chips),
        grid=(11,),
        in_specs=[pl.BlockSpec((rows, ff // 2), lambda s: (0, jnp.minimum(s, 9) // 2)), any_, any_, any_, any_],
        out_specs=[pl.BlockSpec((d // 2, d // 2), block), any_, any_],
        out_shape=[jax.ShapeDtypeStruct((ff + 2 * d, d), BF16), jax.ShapeDtypeStruct((2 * TM, d), BF16),
                   jax.ShapeDtypeStruct((rows // 4, d), BF16)],
        scratch_shapes=[
            pltpu.VMEM((2, rows, d // 2), BF16),
            pltpu.VMEM((2, 2, SUB, d), F32), pltpu.VMEM((2, 2, SUB, d), BF16),
            pltpu.VMEM((6, 2, SUB, d), BF16), pltpu.VMEM((2, 2, SUB, d), BF16),
            pltpu.SemaphoreType.DMA((2, 2)),
            pltpu.SemaphoreType.DMA((2, 2, 2)), pltpu.SemaphoreType.DMA((6, 2)), pltpu.SemaphoreType.DMA((6, 2)),
            pltpu.SemaphoreType.DMA((2, 2)), pltpu.SemaphoreType.DMA((4,)), pltpu.SemaphoreType.DMA((4,)),
        ],
        compiler_params=pltpu.CompilerParams(collective_id=1, has_side_effects=True, vmem_limit_bytes=VMEM_LIMIT,
                                             dimension_semantics=("arbitrary",)),
        cost_estimate=pl.CostEstimate(flops=5 * rows * d * ff, bytes_accessed=12 * rows * d, transcendentals=0),
        name="scatter_and_dw",
    )(act, dyf, xn, own, other)


def call_c(act, xn, xfar, w, dx):
    rows, d = act.shape[0], xn.shape[1]
    ff = act.shape[1] // 3
    near = xn.shape[0]
    cut = 8

    def kernel(xn_ref, xfar_ref, du_ref, wd_ref, wg_ref, wu_ref, dx_ref, dx_out, wg_out, wu_out, wd_out):
        dx_out[...] = dx_ref[...]
        wg_out[...] = wg_ref[...]
        wd_out[...] = wd_ref[...]
        wu_out[:, :ff // 2] = wu_ref[...]
        v = lax.dot_general(xn_ref[...], du_ref[:near], TN, preferred_element_type=F32)
        v = v + lax.dot_general(xfar_ref[...], du_ref[near:], TN, preferred_element_type=F32)
        wu_out[:, ff // 2:] = v.astype(BF16)

    rows_of = lambda size, start=0: pl.BlockSpec((size // cut, d), lambda s: (start + s, 0))
    return pl.pallas_call(
        kernel,
        grid=(cut,),
        in_specs=[
            pl.BlockSpec((near, d // cut), lambda s: (0, s)),
            pl.BlockSpec((rows - near, d // cut), lambda s: (0, s)),
            pl.BlockSpec((rows, ff // 2), lambda s: (0, 5)),
            rows_of(ff), rows_of(d, cut),
            pl.BlockSpec((d // cut, ff // 2), lambda s: (2 * cut + s, 0)),
            rows_of(dx.shape[0]),
        ],
        out_specs=[rows_of(dx.shape[0]), rows_of(d), rows_of(d), rows_of(ff)],
        out_shape=[jax.ShapeDtypeStruct(dx.shape, BF16), jax.ShapeDtypeStruct((d, ff), BF16),
                   jax.ShapeDtypeStruct((d, ff), BF16), jax.ShapeDtypeStruct((ff, d), BF16)],
        compiler_params=pltpu.CompilerParams(vmem_limit_bytes=VMEM_LIMIT, dimension_semantics=("arbitrary",)),
        cost_estimate=pl.CostEstimate(flops=rows * d * ff, bytes_accessed=12 * rows * d, transcendentals=0),
        name="dw_and_results",
    )(xn, xfar, act, w, w, w, dx)


def solution(mesh):
    chips = mesh.shape["tp"] // 2

    def local(x, dy, gate, up, wg, wu, wd):
        dyf, xn, act, own, other = call_a(chips, dy, x, gate, up, wd, wg, wu)
        w, dx, xfar = call_b(chips, act, dyf, xn, own, other)
        return tuple(call_c(act, xn, xfar, w, dx))

    rows, cols = P(("dp", "tp"), None), P("dp", "tp")
    return jax.shard_map(local, mesh=mesh,
                         in_specs=(rows, rows, cols, cols, P(None, "tp"), P(None, "tp"), P("tp", None)),
                         out_specs=(rows, cols, cols, P(("dp", "tp"), None)), check_vma=False)
```
